128 devices in a mesh: wide: 64 (over x, y_hi, z, core), pair: 2 (over y_lo).
Axes of the slice: x: 4, y: 4 (y_hi: 2, y_lo: 2; y = y_hi * 2 + y_lo), z: 4, core: 2. Of those that a mesh axis runs over, the one named last changes fastest.
Arguments:
- pooled_b: bfloat16 [64, 64, 512, 128], P('wide', None, 'pair'), may hold values from -6 to 6
- dense_output_second: bfloat16 [32768, 128], P(('wide', 'pair')), may hold values from -4 to 4
- counts_b: int32 [32768, 26], P(('wide', 'pair')), may hold values from 1 to 8
- slot_of: int32 [64], replicated, may hold values from 0 to 63, each once
- stacked_a: bfloat16 [32768, 3456], P(('wide', 'pair')), may hold values from -4 to 4
- upstream_a: bfloat16 [32768, 3456], P(('wide', 'pair')), may hold values from -6 to 6
- counts_a: int32 [32768, 26], P(('wide', 'pair')), may hold values from 1 to 8
- down_projection: bfloat16 [3456, 512], P('wide'), may hold values from -0.109375 to 0.109375
- proj_up: bfloat16 [512, 3456], P(None, 'wide'), may hold values from -0.25 to 0.25
- cross_layer_bias: bfloat16 [3456], P('wide'), may hold values from -3 to 3
Outputs:
- crossed_b: bfloat16 [32768, 3456], P(('wide', 'pair'))
- dense_grad_a: bfloat16 [32768, 128], P(('wide', 'pair'))
- pooled_grad_a: bfloat16 [64, 64, 512, 128], P('wide', None, 'pair')
- grad_down: float32 [3456, 512], P('wide')
- grad_up: float32 [512, 3456], P(None, 'wide')
- grad_bias: float32 [3456], P('wide')
The draws below stay inside these ranges and needn't reach their ends.
Inputs may be any that keep to these rules, and one draw needn't show every extreme that they name: slot_of holds every slot once; its first 26 entries are the slots of tables 0 to 25, the rest are unused. Slot s lies on index s // 1 of wide.
All inputs are finite; a program needn't handle non-finite values.
Results may differ from the reference program's by a relative error of at most 0.0075.
Values may be sent and summed in bfloat16 or wider, within the bound.
No kernel may reach another device: no remote copies, remote signals or barrier semaphores. Data moves between devices by JAX's collectives and lax.ppermute only.
A program may use at most 128 MiB of HBM per device.

```python
import jax
import jax.numpy as jnp
from jax import lax

E = 128
TABLES = 26
RANK = 512
SAMP = 256
POOL_MAX = 8
WIDTH = 3456
SLOTS = 64
BATCH = 32768
N_WIDE = 64
N_PAIR = 2


def touch_ends(drawn, stream_key, low, largest):
    dims = drawn.shape
    index_at = [jax.random.randint(jax.random.fold_in(stream_key, axis), (), 0, dims[axis]) for axis in range(len(dims))]
    drawn = drawn.at[tuple(index_at)].set(low)
    longest = dims.index(max(dims))
    index_at[longest] = (index_at[longest] + 1) % dims[longest]
    return drawn.at[tuple(index_at)].set(largest)


def raised(values, key, source, target, shards_of, factor):
    owner, partner = [(jnp.arange(values.shape[dim]) // (values.shape[dim] // shards_of)).reshape([-1 if axis == dim else 1 for axis in range(values.ndim)]) for dim in (source, target)]
    chosen = jax.random.permutation(key, shards_of)[partner]
    strong = (owner == chosen) | (owner == (partner + shards_of // 2) % shards_of)
    return jnp.where(strong, factor * values, values)


def block_scale(rng, extent, pieces, least, high):
    gain, own = 1.0, jax.random.fold_in(rng, 6)
    for axis_at, blocks in pieces:
        heights = jnp.exp(jax.random.uniform(jax.random.fold_in(own, axis_at), (blocks,), jnp.float32, least / len(pieces), high / len(pieces)))
        gain = gain * jnp.repeat(heights, extent[axis_at] // blocks).reshape([-1 if axis == axis_at else 1 for axis in range(len(extent))])
    return gain


def noise(rng, shape, spread, reach, split=(), kind=jnp.bfloat16):
    gain = block_scale(rng, shape, split, -0.22, 0.18) if split else 1.0
    drawn = jax.random.normal(rng, shape, jnp.float32) * spread * gain
    return jnp.minimum(jnp.maximum(drawn, -reach), reach).astype(kind)


def gaussian_with(key, dims, spread, limit, pieces, heavy, held_as=jnp.bfloat16):
    array = spread * jax.random.normal(key, dims, jnp.float32)
    if pieces:
        array = array * block_scale(key, dims, pieces, -0.22, 0.18)
    return jnp.clip(raised(array, jax.random.fold_in(key, 3), *heavy), -limit, limit).astype(held_as)


def setup_inputs(seed: int = 0) -> dict:
    keys = jax.random.split(jax.random.key(seed), 11)
    pooled_b = noise(keys[0], (SLOTS, N_WIDE, N_PAIR * SAMP, E), 1.0, 6.0, ((0, 64), (2, 2)))
    dense_output_second = noise(keys[1], (BATCH, E), 0.5, 4.0, ((0, 128),))
    counts_b = touch_ends(jax.random.randint(keys[2], (BATCH, TABLES), 1, POOL_MAX + 1), jax.random.fold_in(keys[2], 1), 1, POOL_MAX).astype(jnp.int32)
    slot_of = jax.random.permutation(keys[3], SLOTS).astype(jnp.int32)
    stacked_a = noise(keys[4], (BATCH, WIDTH), 0.5, 4.0, ((0, 128),))
    upstream_a = gaussian_with(keys[5], (BATCH, WIDTH), 0.25, 6.0, ((0, 128),), (0, 1, 128, 5.5))
    counts_a = touch_ends(jax.random.randint(keys[6], (BATCH, TABLES), 1, POOL_MAX + 1), jax.random.fold_in(keys[6], 1), 1, POOL_MAX).astype(jnp.int32)
    down_projection = noise(keys[7], (WIDTH, RANK), WIDTH ** -0.5, 0.109375, ((0, 64),))
    proj_up = noise(keys[8], (RANK, WIDTH), RANK ** -0.5, 0.25, ((1, 64),))
    cross_layer_bias = noise(keys[9], (WIDTH,), 0.5, 3.0, ((0, 64),))
    return {"pooled_b": pooled_b, "dense_output_second": dense_output_second, "counts_b": counts_b, "slot_of": slot_of, "stacked_a": stacked_a, "upstream_a": upstream_a, "counts_a": counts_a, "down_projection": down_projection, "proj_up": proj_up, "cross_layer_bias": cross_layer_bias}


def table_means(slot_rows, lookup_count, table_slots):
    picked = jnp.take(slot_rows, table_slots, axis=0).astype(jnp.float32)
    scaled = picked / jnp.transpose(lookup_count).astype(jnp.float32)[:, :, None]
    return jnp.transpose(scaled, (1, 0, 2)).reshape(scaled.shape[1], -1).astype(jnp.bfloat16)


def cross_forward(stacked, down, up):
    low_rank = jnp.dot(stacked, down, preferred_element_type=jnp.float32).astype(jnp.bfloat16)
    projected = jnp.dot(low_rank, up, preferred_element_type=jnp.float32)
    return low_rank, projected


def crossed_output(stacked, projected, bias):
    stacked_wide = stacked.astype(jnp.float32)
    return (stacked_wide * (projected + bias.astype(jnp.float32)) + stacked_wide).astype(jnp.bfloat16)


def cross_backward(stacked, upstream, lookup_count, down, up, bias, feature_index):
    low_rank, projected = cross_forward(stacked, down, up)
    stacked_wide = stacked.astype(jnp.float32)
    upstream_wide = upstream.astype(jnp.float32)
    scale_grad = upstream_wide * stacked_wide
    grad_bias = jnp.sum(scale_grad, axis=0)
    proj_grad = scale_grad.astype(jnp.bfloat16)
    over_rows = (((0,), (0,)), ((), ()))
    over_cols = (((1,), (1,)), ((), ()))
    grad_up = lax.dot_general(low_rank, proj_grad, over_rows, preferred_element_type=jnp.float32)
    low_grad = lax.dot_general(proj_grad, up, over_cols, preferred_element_type=jnp.float32).astype(jnp.bfloat16)
    grad_down = lax.dot_general(stacked, low_grad, over_rows, preferred_element_type=jnp.float32)
    input_grad = upstream_wide * (projected + bias.astype(jnp.float32)) + upstream_wide
    input_grad = input_grad + lax.dot_general(low_grad, down, over_cols, preferred_element_type=jnp.float32)
    rows = stacked.shape[0]
    dense_gradient = input_grad[:, :feature_index].astype(jnp.bfloat16)
    table_gradient = input_grad[:, feature_index:].reshape(rows, -1, feature_index) / lookup_count.astype(jnp.float32)[:, :, None]
    table_gradient = jnp.transpose(table_gradient, (1, 0, 2)).astype(jnp.bfloat16)
    return dense_gradient, table_gradient, grad_down, grad_up, grad_bias


def reference(pooled_b, dense_output_second, counts_b, slot_of, stacked_a, upstream_a, counts_a, down_projection, proj_up, cross_layer_bias):
    feature_index = dense_output_second.shape[1]
    table_slots = slot_of[:TABLES].astype(jnp.int32)
    slot_rows = pooled_b.reshape(SLOTS, BATCH, feature_index)

    def per_block(running, block_index):
        first_row = (block_index * SAMP).astype(jnp.int32)
        rows_b = lax.dynamic_slice_in_dim(slot_rows, first_row, SAMP, 1)
        dense_rows = lax.dynamic_slice_in_dim(dense_output_second, first_row, SAMP, 0)
        counts_rows_b = lax.dynamic_slice_in_dim(counts_b, first_row, SAMP, 0)
        stacked_b = jnp.concatenate([dense_rows, table_means(rows_b, counts_rows_b, table_slots)], axis=1)
        low_rank, projected = cross_forward(stacked_b, down_projection, proj_up)
        crossed = crossed_output(stacked_b, projected, cross_layer_bias)
        stacked_rows = lax.dynamic_slice_in_dim(stacked_a, first_row, SAMP, 0)
        upstream_rows = lax.dynamic_slice_in_dim(upstream_a, first_row, SAMP, 0)
        counts_rows_a = lax.dynamic_slice_in_dim(counts_a, first_row, SAMP, 0)
        dense_gradient, table_gradient, grad_d, grad_u, grad_b = cross_backward(
            stacked_rows, upstream_rows, counts_rows_a, down_projection, proj_up, cross_layer_bias, feature_index)
        slot_grad = jnp.zeros((SLOTS, SAMP, feature_index), jnp.bfloat16).at[table_slots].set(table_gradient)
        running = (running[0] + grad_d, running[1] + grad_u, running[2] + grad_b)
        return running, (crossed, dense_gradient, slot_grad)

    initial = (jnp.zeros((WIDTH, RANK), jnp.float32), jnp.zeros((RANK, WIDTH), jnp.float32),
               jnp.zeros((WIDTH,), jnp.float32))
    blocks = jnp.arange(BATCH // SAMP, dtype=jnp.int32)
    totals, (crossed, dense_gradient, slot_grad) = lax.scan(per_block, initial, blocks)
    crossed_b = crossed.reshape(BATCH, WIDTH)
    dense_grad_a = dense_gradient.reshape(BATCH, feature_index)
    pooled_grad_a = jnp.transpose(slot_grad, (1, 0, 2, 3)).reshape(SLOTS, N_WIDE, N_PAIR * SAMP, feature_index)
    return crossed_b, dense_grad_a, pooled_grad_a, totals[0], totals[1], totals[2]
```

```python
import functools
import jax, jax.numpy as jnp
from jax import lax
from jax.experimental import pallas as pl
from jax.experimental.pallas import tpu as pltpu
from jax.sharding import PartitionSpec as P
F32, BF16 = jnp.float32, jnp.bfloat16
AXES = ("wide", "pair")

def flat(x, y, z, c):
    return ((((x * 2 + y // 2) * 4 + z) * 2 + c) * 2) + y % 2

def send(value, dx=0, dy=0, dz=0, dc=0):
    pairs = [
        (flat(x, y, z, c), flat(x ^ dx, y ^ dy, z ^ dz, c ^ dc))
        for x in range(4) for y in range(4) for z in range(4) for c in range(2)
    ]
    return lax.ppermute(value, AXES, pairs)

def whole(n):
    return [pl.BlockSpec(memory_space=pltpu.VMEM)] * n

SCALARS = pl.BlockSpec(memory_space=pltpu.SMEM)

def join_kernel(place, own, ry, rz, ryz, a_ref, b_ref, held, rows):
    yh, zl, c = place[1], place[3], place[4]
    for i, ref in enumerate((own, rz, ry, ryz)):
        for k in range(2):
            held[2 * i + k] = ref[k].astype(F32)
    for y in range(2):
        bias = jnp.zeros((8, 512), F32)
        rows[216:224, :] = bias
        for s in range(4):
            at = 4 * (y ^ yh) + 2 * ((s // 2) ^ zl) + ((s % 2) ^ c)
            rows[54 * s : 54 * s + 54, :] = held[at, 0:54, :]
            line = held[at, 48:56, :]
            line = jnp.where(lax.broadcasted_iota(jnp.int32, (8, 512), 0) == 6, line, 0.0)
            line = pltpu.roll(line, 2, 0)
            bias = bias + (pltpu.roll(line, 54 * s, 1) if s else line)
        rows[216:224, :] = bias
        a_ref[y] = rows[:, 0:256].astype(BF16)
        b_ref[y] = rows[:, 256:512].astype(BF16)

def assemble_kernel(place, *refs):
    w_ref, bias_ref = refs[16], refs[17]
    x, zh = place[0], place[2]
    for i in range(16):
        half, dz, dx = i // 8, (i // 4) % 2, i % 4
        for y in range(2):
            at = (x ^ dx) * 4 + y * 2 + (zh ^ dz)
            w_ref[at, :, 256 * half : 256 * half + 256] = refs[i][y, 0:216, :]
            if half == 0:
                bias_ref[at] = refs[i][y, 216:224, :]

def place_of():
    w = lax.axis_index("wide")
    x, yh, z, c = w // 16, (w // 8) % 2, (w // 2) % 4, w % 2
    return jnp.stack([x, yh, z // 2, z % 2, c]).astype(jnp.int32)

def gather_weights(down, up, bias, place):
    c = place[4]
    tail = jnp.concatenate([jnp.pad(bias, (0, 512 - 54))[None], jnp.zeros((1, 512), BF16)], 0)
    d56 = jnp.concatenate([down, tail], 0)
    u56 = jnp.concatenate([up.T, tail], 0)
    mine = jnp.where(c == 0, d56, u56)
    other = jnp.where(c == 0, u56, d56)
    own = jnp.stack([mine, send(other, dc=1)])
    ry, rz, ryz = send(own, dy=3), send(own, dz=1), send(own, dy=3, dz=1)
    half = jax.ShapeDtypeStruct((2, 224, 256), BF16)
    a, b = pl.pallas_call(
        join_kernel, out_shape=(half, half),
        in_specs=[SCALARS] + whole(4), out_specs=whole(2),
        scratch_shapes=[pltpu.VMEM((8, 56, 512), F32), pltpu.VMEM((224, 512), F32)],
        cost_estimate=pl.CostEstimate(flops=10**6, bytes_accessed=10**6, transcendentals=0),
    )(place, own, ry, rz, ryz)
    az = send(a, dz=2)
    bx = [send(b, dx=d) for d in (1, 2, 3)]
    ax = [send(a, dx=d) for d in (1, 2, 3)]
    bz = send(b, dz=2)
    azx = [send(az, dx=d) for d in (1, 2, 3)]
    bzx = [send(v, dz=2) for v in bx]
    w3, lines = pl.pallas_call(
        assemble_kernel,
        out_shape=(jax.ShapeDtypeStruct((16, 216, 512), BF16), jax.ShapeDtypeStruct((16, 8, 256), BF16)),
        in_specs=[SCALARS] + whole(16), out_specs=whole(2),
        cost_estimate=pl.CostEstimate(flops=10**6, bytes_accessed=7 * 10**6, transcendentals=0),
    )(place, a, *ax, az, *azx, b, *bx, bz, *bzx)
    full_bias = lines[:, 0, :216].reshape(1, 3456)
    return w3, send(w3, dc=1), full_bias


def picked(flag, first, second):
    return jnp.where(flag == 0, first, second)


def reduce_kernel(place, st_ref, up_ref, wc_ref, wo_ref, low_ref, lg_ref, gb_ref, low_acc, lg_acc):
    step, c = pl.program_id(0), place[4]

    @pl.when(step == 0)
    def _():
        low_acc[...] = jnp.zeros_like(low_acc)
        lg_acc[...] = jnp.zeros_like(lg_acc)

    wc, wo = wc_ref[...], wo_ref[...]
    down, up = picked(c, wc, wo), picked(c, wo, wc)
    scale = up_ref[...].astype(F32) * st_ref[...].astype(F32)
    gb_ref[...] = jnp.sum(scale, axis=0, keepdims=True)
    low_acc[...] += jnp.dot(st_ref[...], down, preferred_element_type=F32)
    lg_acc[...] += jnp.dot(scale.astype(BF16), up, preferred_element_type=F32)

    @pl.when(step == pl.num_programs(0) - 1)
    def _():
        low_ref[...] = low_acc[...].astype(BF16)
        lg_ref[...] = lg_acc[...].astype(BF16)


ROWS = (((0,), (0,)), ((), ()))
COLS = (((1,), (1,)), ((), ()))
N = 384


def grads_kernel(place, slots, st_ref, up_ref, wc_ref, wo_ref, low_ref, lg_ref, bias_ref, cnt_ref,
                 keep_ref, send_ref, dense_ref, out_ref):
    step, c = pl.program_id(0), place[4]
    wc, wo = wc_ref[...], wo_ref[...]
    down, up = picked(c, wc, wo), picked(c, wo, wc)
    low, lg, st = low_ref[...], lg_ref[...], st_ref[...]
    upstream = up_ref[...].astype(F32)
    pg = (upstream * st.astype(F32)).astype(BF16)
    gu = lax.dot_general(pg, low, ROWS, preferred_element_type=F32)
    gd = lax.dot_general(st, lg, ROWS, preferred_element_type=F32)
    keep_ref[...] = picked(c, gd, gu).astype(BF16)
    send_ref[...] = picked(c, gu, gd).astype(BF16)
    projected = lax.dot_general(low, up, COLS, preferred_element_type=F32)
    grad = upstream * (projected + bias_ref[...]) + upstream
    grad = grad + lax.dot_general(lg, down, COLS, preferred_element_type=F32)
    lane = lax.broadcasted_iota(jnp.int32, cnt_ref.shape, 1)
    for i in range(3):
        block = 3 * step + i
        count = jnp.sum(jnp.where(lane == block, cnt_ref[...], 0.0), axis=1, keepdims=True)
        value = (grad[:, 128 * i : 128 * i + 128] / count).astype(BF16)
        if i == 0:
            @pl.when(step == 0)
            def _():
                dense_ref[...] = value

            @pl.when(step > 0)
            def _():
                out_ref[slots[block - 1]] = value
        else:
            out_ref[slots[block - 1]] = value
    for k in range(5):
        entry = 26 + 5 * step + k

        @pl.when(entry < 64)
        def _():
            out_ref[slots[entry]] = jnp.zeros((256, 128), BF16)


def forward_kernel(place, slots, p0, p1, p2, dense_ref, cnt_ref, wc_ref, wo_ref, bias_ref,
                   out_ref, held, acc, low):
    step, c = pl.program_id(0), place[4]

    @pl.when(step == 0)
    def _():
        acc[...] = jnp.zeros_like(acc)

    @pl.when(step < 9)
    def _():
        lane = lax.broadcasted_iota(jnp.int32, cnt_ref.shape, 1)
        for i, ref in enumerate((p0, p1, p2)):
            count = jnp.sum(jnp.where(lane == 3 * step + i, cnt_ref[...], 0.0), axis=1, keepdims=True)
            value = (ref[0].astype(F32) / count).astype(BF16)
            if i == 0:
                value = jnp.where(step == 0, dense_ref[...], value)
            held[step, :, 128 * i : 128 * i + 128] = value
        down = picked(c, wc_ref[...], wo_ref[...])
        acc[...] += jnp.dot(held[step], down, preferred_element_type=F32)

    @pl.when(step == 8)
    def _():
        low[...] = acc[...].astype(BF16)

    @pl.when(step >= 9)
    def _():
        up = picked(c, wo_ref[...], wc_ref[...])
        st = held[step - 9].astype(F32)
        projected = lax.dot_general(low[...], up, COLS, preferred_element_type=F32)
        out_ref[...] = (st * (projected + bias_ref[...]) + st).astype(BF16)


def params():
    return pltpu.CompilerParams(dimension_semantics=("arbitrary",), vmem_limit_bytes=60 * 2**20)


def backward(stacked, upstream, counts, wc, wo, bias, place, slots):
    col = lambda j, *_: (0, j)
    row = lambda j, *_: (j, 0)
    fix = lambda j, *_: (0, 0)
    act, wgt = pl.BlockSpec((256, N), col), pl.BlockSpec((N, 512), row)
    low_spec = pl.BlockSpec((256, 512), fix)
    low, lg, gb = pl.pallas_call(
        reduce_kernel,
        out_shape=(jax.ShapeDtypeStruct((256, 512), BF16),) * 2 + (jax.ShapeDtypeStruct((1, 3456), F32),),
        grid_spec=pltpu.PrefetchScalarGridSpec(
            num_scalar_prefetch=1, grid=(9,),
            in_specs=[act, act, wgt, wgt],
            out_specs=[low_spec, low_spec, pl.BlockSpec((1, N), col)],
            scratch_shapes=[pltpu.VMEM((256, 512), F32)] * 2),
        compiler_params=params(),
        cost_estimate=pl.CostEstimate(flops=2 * 10**9, bytes_accessed=11 * 10**6, transcendentals=0),
    )(place, stacked, upstream, wc, wo)
    return low, lg, gb, pl.pallas_call(
        grads_kernel,
        out_shape=(jax.ShapeDtypeStruct((3456, 512), BF16),) * 2
        + (jax.ShapeDtypeStruct((256, 128), BF16), jax.ShapeDtypeStruct((64, 256, 128), BF16)),
        grid_spec=pltpu.PrefetchScalarGridSpec(
            num_scalar_prefetch=2, grid=(9,),
            in_specs=[act, act, wgt, wgt, low_spec, low_spec, pl.BlockSpec((1, N), col),
                      pl.BlockSpec((256, 128), fix)],
            out_specs=[wgt, wgt, pl.BlockSpec((256, 128), fix),
                       pl.BlockSpec((64, 256, 128), lambda j, *_: (0, 0, 0))]),
        compiler_params=params(),
        cost_estimate=pl.CostEstimate(flops=4 * 10**9, bytes_accessed=22 * 10**6, transcendentals=0),
    )(place, slots, stacked, upstream, wc, wo, low, lg, bias, counts)


def forward(arrived, dense, counts, wc, wo, bias, place, slots):
    def piece(i):
        def index(j, place, slots):
            return (slots[jnp.clip(3 * jnp.minimum(j, 8) + i - 1, 0, 25)], 0, 0)
        return pl.BlockSpec((1, 256, 128), index)

    def weight(core):
        def index(j, place, slots):
            first, second = jnp.minimum(j, 8), jnp.maximum(j - 9, 0)
            return (jnp.where(place[4] == core, first, second), 0)
        return pl.BlockSpec((N, 512), index)

    late = lambda j, *_: (0, jnp.maximum(j - 9, 0))
    fix = pl.BlockSpec((256, 128), lambda j, *_: (0, 0))
    return pl.pallas_call(
        forward_kernel,
        out_shape=jax.ShapeDtypeStruct((256, 3456), BF16),
        grid_spec=pltpu.PrefetchScalarGridSpec(
            num_scalar_prefetch=2, grid=(18,),
            in_specs=[piece(0), piece(1), piece(2), fix, fix, weight(0), weight(1),
                      pl.BlockSpec((1, N), late)],
            out_specs=pl.BlockSpec((256, N), late),
            scratch_shapes=[pltpu.VMEM((9, 256, N), BF16), pltpu.VMEM((256, 512), F32),
                            pltpu.VMEM((256, 512), BF16)]),
        compiler_params=params(),
        cost_estimate=pl.CostEstimate(flops=2 * 10**9, bytes_accessed=12 * 10**6, transcendentals=0),
    )(place, slots, arrived, arrived, arrived, dense, counts, wc, wo, bias)


def sum1_kernel(place, keep, recv, b0, b1, a0, a1, a2, a3, own, far):
    x, zh = place[0], place[2]
    for d, ref in enumerate((a0, a1, a2, a3)):
        for q in range(4):
            k = (x ^ d) * 4 + q
            ref[q, 0:216, :] = (keep[k, :, 0:256].astype(F32) + recv[k, :, 0:256].astype(F32)).astype(ref.dtype)
            ref[q, 216:224, :] = (b0[k] + b1[k]).astype(ref.dtype)
    for d, ref in enumerate((own, far)):
        for q in range(8):
            k = q * 2 + (zh ^ d)
            ref[q] = (keep[k, :, 256:512].astype(F32) + recv[k, :, 256:512].astype(F32)).astype(ref.dtype)


def sum2_kernel(place, a0, r1, r2, r3, own, rb, akeep, asend, bkeep, s1, s2, s3):
    x, zh = place[0], place[2]
    for d, ref in enumerate((akeep, asend)):
        for y in range(2):
            q = y * 2 + (zh ^ d)
            total = a0[q] + r1[q].astype(F32) + r2[q].astype(F32) + r3[q].astype(F32)
            ref[y] = total.astype(ref.dtype)
    for d, ref in enumerate((bkeep, s1, s2, s3)):
        for y in range(2):
            q = (x ^ d) * 2 + y
            ref[y] = (own[q] + rb[q].astype(F32)).astype(ref.dtype)


def sum3_kernel(place, akeep, ra, bkeep, r1, r2, r3, own, py, pz, pyz, rows, held):
    yh, zl = place[1], place[3]
    line_row = lax.broadcasted_iota(jnp.int32, (8, 512), 0)
    line_col = lax.broadcasted_iota(jnp.int32, (8, 512), 1)
    rows[216:224, :] = jnp.zeros((8, 512), F32)
    for y in range(2):
        rows[:, 0:256] = akeep[y] + ra[y].astype(F32)
        rows[0:216, 256:512] = bkeep[y] + r1[y].astype(F32) + r2[y].astype(F32) + r3[y].astype(F32)
        bias = rows[216:224, :]
        for s in range(4):
            held[4 * y + s, 0:48, :] = rows[54 * s : 54 * s + 48, :]
            tile = rows[54 * s + 48 : 54 * s + 56, :]
            line = pltpu.roll(bias, 512 - 54 * s, 1) if s else bias
            line = pltpu.roll(jnp.where(line_col < 54, line, 0.0), 6, 0)
            tile = jnp.where(line_row < 6, tile, jnp.where(line_row == 6, line, 0.0))
            held[4 * y + s, 48:56, :] = tile
    for dy, dz, ref in ((0, 0, own), (1, 0, py), (0, 1, pz), (1, 1, pyz)):
        for k in range(2):
            at = 4 * (yh ^ dy) + 2 * (zl ^ dz) + k
            ref[k] = held[at].astype(ref.dtype)


def sum4_kernel(place, own, ry, rz, ryz, mine, other):
    c = place[4]
    for ref, at in ((mine, c), (other, 1 - c)):
        total = own[at] + ry[at].astype(F32) + rz[at].astype(F32) + ryz[at].astype(F32)
        ref[...] = total.astype(BF16)


def summed(kernel, place, ins, outs, scratch=(), flops=10**6):
    shapes = tuple(jax.ShapeDtypeStruct(s, t) for s, t in outs)
    return pl.pallas_call(
        kernel, out_shape=shapes, in_specs=[SCALARS] + whole(len(ins)), out_specs=tuple(whole(len(outs))),
        scratch_shapes=list(scratch),
        compiler_params=pltpu.CompilerParams(vmem_limit_bytes=60 * 2**20),
        cost_estimate=pl.CostEstimate(flops=flops, bytes_accessed=8 * 10**6, transcendentals=0),
    )(place, *ins)


def reduce_first(keep, away, gb, place):
    lines = jnp.pad(gb.reshape(16, 1, 216), ((0, 0), (0, 7), (0, 40)))
    keep, away = keep.reshape(16, 216, 512), away.reshape(16, 216, 512)
    a0, a1, a2, a3, own, far = summed(
        sum1_kernel, place, (keep, send(away, dc=1), lines, send(lines, dc=1)),
        [((4, 224, 256), F32)] + [((4, 224, 256), BF16)] * 3 + [((8, 216, 256), F32), ((8, 216, 256), BF16)])
    ins = (a0, send(a1, dx=1), send(a2, dx=2), send(a3, dx=3), own, send(far, dz=2))
    return summed(
        sum2_kernel, place, ins,
        [((2, 224, 256), F32), ((2, 224, 256), BF16), ((2, 216, 256), F32)] + [((2, 216, 256), BF16)] * 3)


def reduce_rest(parts, place):
    akeep, asend, bkeep, s1, s2, s3 = parts
    ins = (akeep, send(asend, dz=2), bkeep, send(s1, dx=1), send(s2, dx=2), send(s3, dx=3))
    own, py, pz, pyz = summed(
        sum3_kernel, place, ins, [((2, 56, 512), F32)] + [((2, 56, 512), BF16)] * 3,
        [pltpu.VMEM((224, 512), F32), pltpu.VMEM((8, 56, 512), F32)])
    mine, other = summed(
        sum4_kernel, place, (own, send(py, dy=3), send(pz, dz=1), send(pyz, dy=3, dz=1)),
        [((56, 512), BF16)] * 2)
    same = mine.astype(F32) + send(mine, dy=1).astype(F32)
    cross = send(other, dc=1).astype(F32) + send(other, dy=1, dc=1).astype(F32)
    c = place[4]
    return picked(c, same, cross)[:54], picked(c, cross, same)[:54].T, same[54, :54]


def local(pooled_b, dense_b, counts_b, slot_of, stacked_a, upstream_a, counts_a, down, up, bias):
    place = place_of()
    table = lambda n: jnp.pad(n.astype(F32), ((0, 0), (1, 101)), constant_values=1.0)
    wc, wo, full_bias = gather_weights(down, up, bias, place)
    wc, wo, full_bias = wc.reshape(3456, 512), wo.reshape(3456, 512), full_bias.astype(F32)
    pooled_b, wc = lax.optimization_barrier((pooled_b, wc))
    arrived = lax.all_to_all(pooled_b.reshape(64, 256, 128), "wide", 0, 0, tiled=True)
    low, lg, gb, (keep, away, dense_grad, slot_grad) = backward(
        stacked_a, upstream_a, table(counts_a), wc, wo, full_bias, place, slot_of)
    parts = reduce_first(keep, away, gb, place)
    slot_grad, *parts = lax.optimization_barrier((slot_grad, *parts))
    returned = lax.all_to_all(slot_grad, "wide", 0, 0, tiled=True)
    crossed = forward(arrived, dense_b, table(counts_b), wc, wo, full_bias, place, slot_of)
    gd, gu, gbias = reduce_rest(parts, place)
    return crossed, dense_grad, returned.reshape(1, 64, 256, 128), gd, gu, gbias


def solution(mesh):
    both = P(("wide", "pair"), None)
    pooled = P("wide", None, "pair", None)
    return jax.shard_map(
        local, mesh=mesh,
        in_specs=(pooled, both, both, P(), both, both, both, P("wide", None), P(None, "wide"), P("wide")),
        out_specs=(both, both, pooled, P("wide", None), P(None, "wide"), P("wide")),
        check_vma=False,
    )
```
